32 devices in a mesh: gossip: 16 (over z, y, core), mp: 2 (over x).
Axes of the slice: x: 2, y: 2, z: 4, core: 2. Of those that a mesh axis runs over, the one named last changes fastest.
Arguments:
- params: float32 [16, 1024, 4096], P('gossip', None, 'mp'), may hold values from -6 to 6
- public: float32 [16, 1024, 64], P('gossip'), may hold values from -12 to 12
- gradients: bfloat16 [2, 16, 1024, 4096], P(None, 'gossip', None, 'mp'), may hold values from -130 to 130
- projection: float32 [4096, 64], P('mp'), may hold values from -0.09375 to 0.09375
- partners: int32 [2, 16], P(None, 'gossip'), may hold values from 0 to 15, as said below
Outputs:
- params_out: float32 [16, 1024, 4096], P('gossip', None, 'mp')
- public_out: float32 [16, 1024, 64], P('gossip')
- consensus: float32 [2], replicated
- grad_norm: float32 [2], replicated
The draws below stay inside these ranges and needn't reach their ends.
Inputs may be any that keep to these rules, and one draw needn't show every extreme that they name: Each row is a pairing of the 16 replicas: partners[r, partners[r, i]] = i and partners[r, i] != i.
All inputs are finite; a program needn't handle non-finite values.
Results may differ from the reference program's by a relative error of at most 0.008.
Values may be sent and summed in bfloat16 or wider, within the bound.
A program may use at most 64 MiB of HBM per device.

```python
import math
import jax
import jax.numpy as jnp
from jax import lax

SLAB = 4096
RANK = 64
ROWS = 1024
ROUNDS = 2
NODES = 16


def draw_gradients(key, part):
    keys = jax.random.split(key, 5)
    shape = (ROUNDS, NODES, ROWS, SLAB)
    row_scale = jnp.exp(jax.random.uniform(keys[0], (ROUNDS, NODES, ROWS, 1), jnp.float32, math.log(0.3), math.log(3.0)))
    col_scale = jnp.exp(jax.random.uniform(keys[1], (ROUNDS, 1, 1, SLAB), jnp.float32, math.log(0.3), math.log(3.0)))
    node_scale = jnp.exp(jnp.linspace(0.0, math.log(3.0), NODES)).reshape(1, NODES, 1, 1)
    base = jnp.clip(jax.random.normal(keys[4], shape, jnp.float32), -4.0, 4.0)
    return (base * row_scale * col_scale * node_scale).astype(jnp.bfloat16)


def draw_public(key, part):
    keys = jax.random.split(key, 3)
    shape = (NODES, ROWS, RANK)
    node_scale = jnp.exp(jnp.linspace(0.0, math.log(3.0), NODES)).reshape(NODES, 1, 1)
    base = jnp.clip(jax.random.normal(keys[2], shape, jnp.float32), -4.0, 4.0)
    return (base * node_scale).astype(jnp.float32)


def draw_partners(key, part):
    rows_list = []
    for round_index in range(ROUNDS):
        order = jax.random.permutation(jax.random.fold_in(key, 71 + round_index), NODES).astype(jnp.int32)
        first = order[0::2]
        second = order[1::2]
        paired = jnp.zeros((NODES,), jnp.int32).at[first].set(second).at[second].set(first)
        rows_list.append(paired)
    return jnp.stack(rows_list)


def steps_of(key, dims, pieces, least, high):
    factor_of = 1.0
    for axis_at, blocks in pieces:
        draws = jax.random.uniform(jax.random.fold_in(jax.random.fold_in(key, 6), axis_at), (blocks,), jnp.float32, least / len(pieces), high / len(pieces))
        factor_of = factor_of * jnp.repeat(jnp.exp(draws), dims[axis_at] // blocks).reshape((-1,) + (1,) * (len(dims) - 1 - axis_at))
    return factor_of


def normal_values(own_key, dims, deviation, reach, cuts=(), kind=jnp.bfloat16):
    drawn = jax.random.normal(own_key, dims, jnp.float32) * deviation
    if len(cuts) > 0:
        drawn = steps_of(own_key, dims, cuts, -0.22, 0.18) * drawn
    return jnp.clip(drawn, min=-reach, max=reach).astype(kind)


def setup_inputs(seed: int = 0) -> dict:
    arg_keys = jax.random.split(jax.random.key(seed), 6)
    return {
        "params": normal_values(arg_keys[0], (NODES, ROWS, SLAB), 1.0, 6.0, ((0, 16), (2, 2)), jnp.float32),
        "public": draw_public(jax.random.fold_in(arg_keys[5], 71), 0),
        "gradients": draw_gradients(jax.random.fold_in(arg_keys[5], 71), 0),
        "projection": normal_values(arg_keys[3], (SLAB, RANK), SLAB ** -0.5, 0.09375, ((0, 2),), jnp.float32),
        "partners": draw_partners(jax.random.fold_in(arg_keys[5], 71), 0),
    }


step_size = 1.0
clip_limit = 0.5
mixing = 0.4
epsilon = 1e-06

def reference(params, public, gradients, projection, partners):
    highest = lax.Precision.HIGHEST
    total = NODES * ROWS * SLAB
    weights = params
    public_state = public
    drift_list = []
    norm_list = []
    for round_index in range(ROUNDS):
        grad_round = gradients[round_index]
        squares = jnp.sum(lax.map(lambda block: jnp.sum(jnp.square(block.astype(jnp.float32))), grad_round))
        norm_value = jnp.sqrt(squares / total + epsilon)
        scale = jnp.minimum(1.0, clip_limit / norm_value)

        def coefficients(item):
            node_weights, node_grad, node_coef = item
            half = node_weights - step_size * scale * node_grad.astype(jnp.float32)
            rebuilt = jnp.dot(node_coef, projection.T, precision=highest)
            return node_coef + jnp.dot(half - rebuilt, projection, precision=highest)
        coef = lax.map(coefficients, (weights, grad_round, public_state))
        sent = coef.astype(jnp.bfloat16)
        mate = jnp.take(sent, partners[round_index], axis=0)
        public_state = sent.astype(jnp.float32)

        def blend(item):
            node_weights, node_grad, own_coef, other_coef = item
            half = node_weights - step_size * scale * node_grad.astype(jnp.float32)
            drift = jnp.dot(other_coef.astype(jnp.float32) - own_coef, projection.T, precision=highest)
            return (half + mixing * drift, jnp.sum(drift * drift))
        weights, terms = lax.map(blend, (weights, grad_round, public_state, mate))
        drift_list.append(jnp.sum(terms) / total)
        norm_list.append(norm_value)
    return (weights, public_state, jnp.stack(drift_list), jnp.stack(norm_list))
```

```python
import functools

import jax
import jax.numpy as jnp
from jax import lax
from jax.experimental import pallas as pl
from jax.experimental.pallas import tpu as pltpu
from jax.sharding import PartitionSpec as P

ROUNDS = 2
step_size = 1.0
clip_limit = 0.5
mixing = 0.4
epsilon = 1e-06

F32 = jnp.float32
BF16 = jnp.bfloat16
HIGHEST = lax.Precision.HIGHEST
VMEM = pl.BlockSpec(memory_space=pltpu.VMEM)
SMEM = pl.BlockSpec(memory_space=pltpu.SMEM)


def high_low(value):
    high = value.astype(BF16)
    return high, (value - high.astype(F32)).astype(BF16)


def dot(a, b):
    return jnp.dot(a, b, preferred_element_type=F32)


def project(mp, w_ref, g_ref, c_ref, p_ref, a_ref, b_ref, d_ref, gram_ref, sq_ref, basis, mixer):
    rank = p_ref.shape[1]
    tile, columns = w_ref.shape[1:]

    @pl.when(pl.program_id(0) == 0)
    def _():
        high, low = high_low(p_ref[...])
        basis[...] = jnp.concatenate([high, low], axis=1)
        parts = lax.dot_general(basis[...], basis[...], (((0,), (0,)), ((), ())), preferred_element_type=F32)
        folded = parts + pltpu.roll(parts, rank, 1)
        gram = folded[:rank] + folded[rank:]
        row = lax.broadcasted_iota(jnp.int32, gram.shape, 0)
        col = lax.broadcasted_iota(jnp.int32, gram.shape, 1)
        gram = jnp.where(col < rank, gram, 0.0)
        gram_ref[...] = gram
        mixer[...] = jnp.where(row == col, 1.0 / mp, 0.0) - gram
        sq_ref[...] = jnp.zeros_like(sq_ref)

    def fold(value):
        return value + pltpu.roll(value, rank, 1)

    for index in range(ROUNDS):
        grad = g_ref[index, 0]
        wide = grad.astype(F32)
        sq_ref[index] += jnp.sum((wide * wide).reshape(tile // 8, 8, columns), axis=0)
        product = fold(dot(grad, basis[...]))
        if index == 0:
            b_ref[...] = product
        else:
            lane = lax.broadcasted_iota(jnp.int32, product.shape, 1)
            d_ref[...] = jnp.where(lane < rank, 0.0, product)
    high, low = high_low(w_ref[0])
    product = fold(dot(high, basis[...]) + dot(low, basis[...]))
    a_ref[...] = product + jnp.dot(c_ref[0], mixer[...], precision=HIGHEST, preferred_element_type=F32)


def exchange(groups, members, total, a_ref, b_ref, d_ref, gram_ref, sq_ref, partners_ref, f_ref, stat_ref,
             tiles, tiles_mp, grams, local, arrived, owned, first, reply, second, final, cons, cons_mp,
             send_g, recv_g, send_m, recv_m):
    g = lax.axis_index("gossip")
    m = lax.axis_index("mp")
    rows = owned.shape[1]
    lanes = owned.shape[2]
    rank = lanes // 2
    flat = groups * rows

    def peers(count, here, act):
        lax.fori_loop(1, count, lambda k, _: (act(lax.rem(here + k, count)), 0)[1], 0)

    barrier = pltpu.get_barrier_semaphore()

    def greet(axis):
        def act(peer):
            pl.semaphore_signal(barrier, inc=1, device_id={axis: peer}, device_id_type=pl.DeviceIdType.MESH)
        return act

    peers(groups, g, greet("gossip"))
    peers(members, m, greet("mp"))

    def copy(axis, slot, src, dst, peer, into):
        send, recv = (send_g, recv_g) if axis == "gossip" else (send_m, recv_m)
        return pltpu.make_async_remote_copy(
            src_ref=src, dst_ref=dst, send_sem=send.at[slot, peer], recv_sem=recv.at[slot, into],
            device_id={axis: peer}, device_id_type=pl.DeviceIdType.MESH)

    def start(axis, slot, source, target):
        count, here = (groups, g) if axis == "gossip" else (members, m)
        peers(count, here, lambda p: copy(axis, slot, source(p), target.at[here], p, here).start())

    def finish(axis, slot, source, target):
        count, here = (groups, g) if axis == "gossip" else (members, m)
        peers(count, here, lambda p: copy(axis, slot, source(p), target.at[p], p, p).wait())

    row = lax.broadcasted_iota(jnp.int32, (8, 128), 0)
    tile = jnp.where(row == 0, jnp.sum(sq_ref[0]), jnp.sum(sq_ref[1]))
    tile = jnp.where(row == 2, partners_ref[0, 0].astype(F32), tile)
    tile = jnp.where(row == 3, partners_ref[1, 0].astype(F32), tile)
    tiles[g] = tile
    grams[m] = gram_ref[...]
    pl.semaphore_wait(barrier, groups - 1 + members - 1)

    start("gossip", 0, lambda p: tiles.at[g], tiles)
    start("mp", 0, lambda p: grams.at[m], grams)
    finish("gossip", 0, lambda p: tiles.at[g], tiles)
    tiles_mp[m] = jnp.sum(tiles[...], axis=0)
    start("mp", 1, lambda p: tiles_mp.at[m], tiles_mp)
    finish("mp", 1, lambda p: tiles_mp.at[m], tiles_mp)
    norm = jnp.sqrt(jnp.sum(tiles_mp[...], axis=0) / total + epsilon)
    scale = step_size * jnp.minimum(1.0, clip_limit / norm)

    local[...] = a_ref[...] - scale[0:1, :] * b_ref[...] - scale[1:2, :] * d_ref[...]
    start("mp", 2, lambda p: local.at[p], arrived)
    summed = local[m]
    finish("mp", 2, lambda p: local.at[p], arrived)
    arrived[m] = summed
    summed = arrived[0]
    for index in range(1, members):
        summed = summed + arrived[index]
    lane = lax.broadcasted_iota(jnp.int32, summed.shape, 2)
    owned[...] = jnp.where(lane < rank, summed.astype(BF16).astype(F32), summed)
    start("gossip", 1, lambda p: owned.at[p], first)
    first[g] = owned[g]

    finish("mp", 0, lambda p: grams.at[m], grams)
    gram = jnp.sum(grams[...], axis=0)[:, :rank]
    inside = lax.broadcasted_iota(jnp.int32, (rows, flat), 0).astype(F32)
    column = lax.broadcasted_iota(jnp.int32, (rows, flat), 1).astype(F32)
    choose = []
    for index in range(ROUNDS):
        blocks = []
        for replica in range(groups):
            wanted = tiles[replica, 2 + index : 3 + index, 0:1] * float(rows) + inside
            blocks.append(jnp.where(wanted == column, 1.0, 0.0))
        choose.append(jnp.concatenate(blocks, axis=0).astype(BF16))
    finish("gossip", 1, lambda p: owned.at[p], first)

    def through(value):
        return jnp.dot(value, gram, precision=HIGHEST, preferred_element_type=F32)

    state = first[...].reshape(flat, lanes)
    sent = state[:, :rank]
    apart = dot(choose[0], sent.astype(BF16)) - sent
    seen = through(apart)
    spread = [jnp.sum(apart * seen)]
    again = (state[:, rank:] + sent + mixing * seen - through(sent)).astype(BF16)
    sent = again.astype(F32)
    later = dot(choose[1], again) - sent
    spread.append(jnp.sum(later * through(later)))
    answer = jnp.concatenate([mixing * (apart + later), sent], axis=1)
    reply[...] = answer.reshape(groups, rows, lanes)
    cons[g] = jnp.where(row == 0, spread[0], spread[1])
    start("gossip", 2, lambda p: reply.at[p], second)
    start("gossip", 3, lambda p: cons.at[g], cons)
    second[g] = reply[g]
    finish("gossip", 2, lambda p: reply.at[p], second)
    start("mp", 3, lambda p: second, final)
    finish("gossip", 3, lambda p: cons.at[g], cons)
    cons_mp[m] = jnp.sum(cons[...], axis=0)
    start("mp", 4, lambda p: cons_mp.at[m], cons_mp)
    final[m] = second[...]
    finish("mp", 3, lambda p: second, final)
    finish("mp", 4, lambda p: cons_mp.at[m], cons_mp)
    f_ref[...] = final[...]
    drift = jnp.sum(cons_mp[...], axis=0) / total
    stat_ref[0] = norm
    stat_ref[1] = scale
    stat_ref[2] = drift


def blend(scale_ref, w_ref, g_ref, f_ref, p_ref, out_ref, basis):
    rank = p_ref.shape[1]

    @pl.when(pl.program_id(0) == 0)
    def _():
        high, low = high_low(p_ref[...])
        basis[...] = jnp.concatenate([high, high, low], axis=1)

    high, low = high_low(f_ref[:, :rank])
    lead = jnp.concatenate([high, low, high], axis=1)
    term = lax.dot_general(lead, basis[...], (((1,), (1,)), ((), ())), preferred_element_type=F32)
    half = w_ref[0] - scale_ref[0] * g_ref[0, 0].astype(F32) - scale_ref[1] * g_ref[1, 0].astype(F32)
    out_ref[0] = half + term


def body(params, public, gradients, projection, partners):
    groups = lax.axis_size("gossip")
    members = lax.axis_size("mp")
    _, height, columns = params.shape
    rank = projection.shape[1]
    lanes = 2 * rank
    total = groups * height * columns * members
    tile = min(128, height)
    steps = height // tile
    rows = height // (groups * members)

    w_spec = pl.BlockSpec((1, tile, columns), lambda i: (0, i, 0))
    g_spec = pl.BlockSpec((ROUNDS, 1, tile, columns), lambda i: (0, 0, i, 0))
    p_spec = pl.BlockSpec((columns, rank), lambda i: (0, 0))
    row_spec = pl.BlockSpec((tile, lanes), lambda i: (i, 0))
    product = jax.ShapeDtypeStruct((height, lanes), F32)
    a, b, d, gram, squares = pl.pallas_call(
        functools.partial(project, members),
        grid=(steps,),
        in_specs=[w_spec, g_spec, pl.BlockSpec((1, tile, rank), lambda i: (0, i, 0)), p_spec],
        out_specs=[row_spec, row_spec, row_spec,
                   pl.BlockSpec((rank, lanes), lambda i: (0, 0)),
                   pl.BlockSpec((ROUNDS, 8, columns), lambda i: (0, 0, 0))],
        out_shape=[product, product, product,
                   jax.ShapeDtypeStruct((rank, lanes), F32),
                   jax.ShapeDtypeStruct((ROUNDS, 8, columns), F32)],
        scratch_shapes=[pltpu.VMEM((columns, lanes), BF16), pltpu.VMEM((rank, lanes), F32)],
        compiler_params=pltpu.CompilerParams(dimension_semantics=("arbitrary",)),
        name="project",
    )(params, gradients, public, projection)

    split = (members, groups, rows, lanes)
    pieces = (groups, rows, lanes)
    final, stats = pl.pallas_call(
        functools.partial(exchange, groups, members, total),
        in_specs=[VMEM] * 5 + [SMEM],
        out_specs=[VMEM, VMEM],
        out_shape=[jax.ShapeDtypeStruct(split, F32), jax.ShapeDtypeStruct((3, 8, 128), F32)],
        scratch_shapes=[
            pltpu.VMEM((groups, 8, 128), F32),
            pltpu.VMEM((members, 8, 128), F32),
            pltpu.VMEM((members, rank, lanes), F32),
            pltpu.VMEM(split, F32),
            pltpu.VMEM(split, F32),
            pltpu.VMEM(pieces, F32),
            pltpu.VMEM(pieces, F32),
            pltpu.VMEM(pieces, F32),
            pltpu.VMEM(pieces, F32),
            pltpu.VMEM(split, F32),
            pltpu.VMEM((groups, 8, 128), F32),
            pltpu.VMEM((members, 8, 128), F32),
            pltpu.SemaphoreType.DMA((4, groups)),
            pltpu.SemaphoreType.DMA((4, groups)),
            pltpu.SemaphoreType.DMA((5, members)),
            pltpu.SemaphoreType.DMA((5, members)),
        ],
        compiler_params=pltpu.CompilerParams(collective_id=0, has_side_effects=True),
        name="exchange",
    )(a.reshape(split), b.reshape(split), d.reshape(split), gram, squares, partners)

    final = final.reshape(height, lanes)
    weights = pl.pallas_call(
        blend,
        grid=(steps,),
        in_specs=[SMEM, w_spec, g_spec, row_spec, p_spec],
        out_specs=w_spec,
        out_shape=jax.ShapeDtypeStruct(params.shape, F32),
        scratch_shapes=[pltpu.VMEM((columns, 3 * rank), BF16)],
        compiler_params=pltpu.CompilerParams(dimension_semantics=("arbitrary",)),
        name="blend",
    )(stats[1, :ROUNDS, 0], params, gradients, final, projection)
    return (weights, final[None, :, rank:], stats[2, :ROUNDS, 0], stats[0, :ROUNDS, 0])


def solution(mesh):
    return jax.shard_map(
        body,
        mesh=mesh,
        in_specs=(
            P("gossip", None, "mp"),
            P("gossip", None, None),
            P(None, "gossip", None, "mp"),
            P("mp", None),
            P(None, "gossip"),
        ),
        out_specs=(P("gossip", None, "mp"), P("gossip", None, None), P(), P()),
        check_vma=False,
    )
```

```python
import functools

import jax
import jax.numpy as jnp
from jax import lax
from jax.experimental import pallas as pl
from jax.experimental.pallas import tpu as pltpu
from jax.sharding import PartitionSpec as P

ROUNDS = 2
step_size = 1.0
clip_limit = 0.5
mixing = 0.4
epsilon = 1e-06

F32 = jnp.float32
BF16 = jnp.bfloat16
HIGHEST = lax.Precision.HIGHEST
VMEM = pl.BlockSpec(memory_space=pltpu.VMEM)
SMEM = pl.BlockSpec(memory_space=pltpu.SMEM)


def high_low(value):
    high = value.astype(BF16)
    return high, (value - high.astype(F32)).astype(BF16)


def dot(a, b):
    return jnp.dot(a, b, preferred_element_type=F32)


def dot_t(a, b):
    return lax.dot_general(a, b, (((1,), (1,)), ((), ())), preferred_element_type=F32)


def exchange(groups, members, total, w_hbm, g_hbm, c_ref, p_ref, partners_ref, half_hbm, f_ref, stat_ref,
             wv, gv, basis, squares, a_ref, b_ref, d_ref,
             tiles, tiles_mp, grams, local, arrived, owned, first, reply, second, final, cons, cons_mp,
             send_g, recv_g, send_m, recv_m, send_u, recv_u, send_f, recv_f, load_g, load_w, store_w):
    g = lax.axis_index("gossip")
    m = lax.axis_index("mp")
    rows = owned.shape[1]
    lanes = owned.shape[2]
    rank = lanes // 2
    flat = groups * rows
    height, columns = wv.shape
    steps = load_w.shape[0]
    chunk = height // steps

    def span(i):
        return pl.ds(pl.multiple_of(i * chunk, chunk), chunk)

    def each(low, high, act):
        lax.fori_loop(low, high, lambda i, _: (act(i), 0)[1], 0)

    def grad_copy(i):
        return pltpu.make_async_copy(g_hbm.at[:, 0, span(i)], gv.at[:, span(i)], load_g.at[i])

    def weight_copy(i):
        return pltpu.make_async_copy(w_hbm.at[0, span(i)], wv.at[span(i)], load_w.at[i])

    def half_copy(i):
        return pltpu.make_async_copy(wv.at[span(i)], half_hbm.at[0, span(i)], store_w.at[i])

    each(0, steps, lambda i: grad_copy(i).start())
    each(0, steps, lambda i: weight_copy(i).start())

    def peers(count, here, act):
        each(1, count, lambda k: act(lax.rem(here + k, count)))

    barrier = pltpu.get_barrier_semaphore()

    def greet(axis):
        def act(peer):
            pl.semaphore_signal(barrier, inc=1, device_id={axis: peer}, device_id_type=pl.DeviceIdType.MESH)
        return act

    peers(groups, g, greet("gossip"))
    peers(members, m, greet("mp"))

    def copy(axis, slot, src, dst, peer, into):
        send, recv = (send_g, recv_g) if axis == "gossip" else (send_m, recv_m)
        return pltpu.make_async_remote_copy(
            src_ref=src, dst_ref=dst, send_sem=send.at[slot, peer], recv_sem=recv.at[slot, into],
            device_id={axis: peer}, device_id_type=pl.DeviceIdType.MESH)

    def start(axis, slot, source, target):
        count, here = (groups, g) if axis == "gossip" else (members, m)
        peers(count, here, lambda p: copy(axis, slot, source(p), target.at[here], p, here).start())

    def finish(axis, slot, source, target):
        count, here = (groups, g) if axis == "gossip" else (members, m)
        peers(count, here, lambda p: copy(axis, slot, source(p), target.at[p], p, p).wait())

    def part_copy(p, q, into):
        return pltpu.make_async_remote_copy(
            src_ref=local.at[q, p], dst_ref=arrived.at[into, p], send_sem=send_u.at[p, q], recv_sem=recv_u.at[p, into],
            device_id={"mp": q}, device_id_type=pl.DeviceIdType.MESH)

    def result_copy(p, q, into):
        return pltpu.make_async_remote_copy(
            src_ref=second.at[p], dst_ref=final.at[into, p], send_sem=send_f.at[p, q], recv_sem=recv_f.at[p, into],
            device_id={"mp": q}, device_id_type=pl.DeviceIdType.MESH)

    high, low = high_low(p_ref[...])
    basis[...] = jnp.concatenate([high, low], axis=0)
    parts = dot_t(basis[...], basis[...])
    folded = parts + pltpu.roll(parts, rank, 1)
    gram = folded[:rank] + folded[rank:]
    gram_row = lax.broadcasted_iota(jnp.int32, gram.shape, 0)
    gram_col = lax.broadcasted_iota(jnp.int32, gram.shape, 1)
    gram = jnp.where(gram_col < rank, gram, 0.0)
    mixer = jnp.where(gram_row == gram_col, 1.0 / members, 0.0) - gram
    a_ref[...] = lax.dot_general(c_ref[...], mixer, (((0,), (0,)), ((), ())), precision=HIGHEST,
                                 preferred_element_type=F32)
    squares[...] = jnp.zeros_like(squares)
    grams[m] = gram

    def fold(value):
        return value + pltpu.roll(value, rank, 1)

    def grad_step(i):
        grad_copy(i).wait()
        for index in range(ROUNDS):
            grad = gv[index, span(i)]
            wide = grad.astype(F32)
            squares[index] += jnp.sum((wide * wide).reshape(chunk // 8, 8, columns), axis=0)
            product = fold(dot_t(grad, basis[...]))
            if index == 0:
                b_ref[span(i)] = product
            else:
                lane = lax.broadcasted_iota(jnp.int32, product.shape, 1)
                d_ref[span(i)] = jnp.where(lane < rank, 0.0, product)

    def weight_step(i):
        weight_copy(i).wait()
        high, low = high_low(wv[span(i)])
        a_ref[span(i)] += fold(dot_t(high, basis[...]) + dot_t(low, basis[...]))

    each(0, steps, grad_step)
    row = lax.broadcasted_iota(jnp.int32, (8, 128), 0)
    tile = jnp.where(row == 0, jnp.sum(squares[0]), jnp.sum(squares[1]))
    tile = jnp.where(row == 2, partners_ref[0].astype(F32), tile)
    tile = jnp.where(row == 3, partners_ref[1].astype(F32), tile)
    tiles[g] = tile
    pl.semaphore_wait(barrier, groups - 1 + members - 1)

    start("gossip", 0, lambda p: tiles.at[g], tiles)
    start("mp", 0, lambda p: grams.at[m], grams)
    each(0, steps // 2, weight_step)
    finish("gossip", 0, lambda p: tiles.at[g], tiles)
    tiles_mp[m] = jnp.sum(tiles[...], axis=0)
    start("mp", 1, lambda p: tiles_mp.at[m], tiles_mp)
    each(steps // 2, steps, weight_step)
    finish("mp", 1, lambda p: tiles_mp.at[m], tiles_mp)
    norm = jnp.sqrt(jnp.sum(tiles_mp[...], axis=0) / total + epsilon)
    scale = step_size * jnp.minimum(1.0, clip_limit / norm)

    local[...] = (a_ref[...] - scale[0:1, :] * b_ref[...] - scale[1:2, :] * d_ref[...]).reshape(local.shape)
    each(1, groups + 1, lambda k: peers(members, m, lambda q: part_copy(lax.rem(g + k, groups), q, m).start()))
    lane = lax.broadcasted_iota(jnp.int32, (rows, lanes), 1)

    def take(p):
        peers(members, m, lambda q: part_copy(p, q, q).wait_recv())
        summed = local[m, p]
        for index in range(1, members):
            summed = summed + arrived[lax.rem(m + index, members), p]
        return jnp.where(lane < rank, summed.astype(BF16).astype(F32), summed)

    def pass_on(p):
        owned[p] = take(p)
        copy("gossip", 1, owned.at[p], first.at[g], p, g).start()

    peers(groups, g, pass_on)
    first[g] = take(g)

    def half_step(i):
        wide = [gv[index, span(i)].astype(F32) for index in range(ROUNDS)]
        wv[span(i)] = wv[span(i)] - scale[0, 0] * wide[0] - scale[1, 0] * wide[1]
        half_copy(i).start()

    each(0, steps, half_step)

    finish("mp", 0, lambda p: grams.at[m], grams)
    gram = jnp.sum(grams[...], axis=0)[:, :rank]
    inside = lax.broadcasted_iota(jnp.int32, (rows, flat), 0).astype(F32)
    column = lax.broadcasted_iota(jnp.int32, (rows, flat), 1).astype(F32)
    choose = []
    for index in range(ROUNDS):
        blocks = []
        for replica in range(groups):
            wanted = tiles[replica, 2 + index : 3 + index, 0:1] * float(rows) + inside
            blocks.append(jnp.where(wanted == column, 1.0, 0.0))
        choose.append(jnp.concatenate(blocks, axis=0).astype(BF16))
    finish("gossip", 1, lambda p: owned.at[p], first)

    def through(value):
        return jnp.dot(value, gram, precision=HIGHEST, preferred_element_type=F32)

    state = first[...].reshape(flat, lanes)
    sent = state[:, :rank]
    apart = dot(choose[0], sent.astype(BF16)) - sent
    seen = through(apart)
    spread = [jnp.sum(apart * seen)]
    again = (state[:, rank:] + sent + mixing * seen - through(sent)).astype(BF16)
    sent = again.astype(F32)
    later = dot(choose[1], again) - sent
    spread.append(jnp.sum(later * through(later)))
    answer = jnp.concatenate([mixing * (apart + later), sent], axis=1)
    reply[...] = answer.reshape(groups, rows, lanes)
    cons[g] = jnp.where(row == 0, spread[0], spread[1])
    start("gossip", 2, lambda p: reply.at[p], second)
    start("gossip", 3, lambda p: cons.at[g], cons)
    second[g] = reply[g]
    final[m, g] = reply[g]
    peers(members, m, lambda q: result_copy(g, q, m).start())

    def hand_over(p):
        copy("gossip", 2, reply.at[p], second.at[p], p, p).wait()
        final[m, p] = second[p]
        peers(members, m, lambda q: result_copy(p, q, m).start())

    peers(groups, g, hand_over)
    finish("gossip", 3, lambda p: cons.at[g], cons)
    cons_mp[m] = jnp.sum(cons[...], axis=0)
    start("mp", 4, lambda p: cons_mp.at[m], cons_mp)
    each(0, steps, lambda i: half_copy(i).wait())
    each(0, groups, lambda p: peers(members, m, lambda q: part_copy(p, q, q).wait_send()))
    each(0, groups, lambda p: peers(members, m, lambda q: result_copy(p, q, q).wait()))
    finish("mp", 4, lambda p: cons_mp.at[m], cons_mp)
    f_ref[...] = final[...]
    drift = jnp.sum(cons_mp[...], axis=0) / total
    stat_ref[0] = norm
    stat_ref[1] = scale
    stat_ref[2] = drift


def blend(h_ref, f_ref, p_ref, stat_ref, out_ref, c_ref, drift_ref, norm_ref, basis):
    rank = p_ref.shape[0]

    @pl.when(pl.program_id(0) == 0)
    def _():
        high, low = high_low(p_ref[...])
        basis[...] = jnp.concatenate([high, high, low], axis=0)
        for index in range(ROUNDS):
            norm_ref[index] = jnp.max(stat_ref[0, index : index + 1, :])
            drift_ref[index] = jnp.max(stat_ref[2, index : index + 1, :])

    high, low = high_low(f_ref[:, :rank])
    out_ref[0] = h_ref[0] + dot(jnp.concatenate([high, low, high], axis=1), basis[...])
    c_ref[...] = f_ref[...].T[rank:]


def body(params, public, gradients, projection, partners):
    groups = lax.axis_size("gossip")
    members = lax.axis_size("mp")
    _, height, columns = params.shape
    rank = projection.shape[1]
    lanes = 2 * rank
    total = groups * height * columns * members
    tile = min(128, height)
    steps = height // tile
    rows = height // (groups * members)
    split = (members, groups, rows, lanes)
    pieces = (groups, rows, lanes)
    basis = projection.T
    anywhere = pl.BlockSpec(memory_space=pl.ANY)
    dma = pltpu.SemaphoreType.DMA
    half, final, stats = pl.pallas_call(
        functools.partial(exchange, groups, members, total),
        in_specs=[anywhere, anywhere, VMEM, VMEM, SMEM],
        out_specs=[anywhere, VMEM, VMEM],
        out_shape=[jax.ShapeDtypeStruct(params.shape, F32), jax.ShapeDtypeStruct(split, F32),
                   jax.ShapeDtypeStruct((3, 8, 128), F32)],
        scratch_shapes=[
            pltpu.VMEM((height, columns), F32),
            pltpu.VMEM((ROUNDS, height, columns), BF16),
            pltpu.VMEM((lanes, columns), BF16),
            pltpu.VMEM((ROUNDS, 8, columns), F32),
            pltpu.VMEM((height, lanes), F32),
            pltpu.VMEM((height, lanes), F32),
            pltpu.VMEM((height, lanes), F32),
            pltpu.VMEM((groups, 8, 128), F32),
            pltpu.VMEM((members, 8, 128), F32),
            pltpu.VMEM((members, rank, lanes), F32),
            pltpu.VMEM(split, F32),
            pltpu.VMEM(split, F32),
            pltpu.VMEM(pieces, F32),
            pltpu.VMEM(pieces, F32),
            pltpu.VMEM(pieces, F32),
            pltpu.VMEM(pieces, F32),
            pltpu.VMEM(split, F32),
            pltpu.VMEM((groups, 8, 128), F32),
            pltpu.VMEM((members, 8, 128), F32),
            dma((4, groups)), dma((4, groups)), dma((5, members)), dma((5, members)),
            dma((groups, members)), dma((groups, members)), dma((groups, members)), dma((groups, members)),
            dma((steps,)), dma((steps,)), dma((steps,)),
        ],
        compiler_params=pltpu.CompilerParams(collective_id=0, has_side_effects=True),
        name="exchange",
    )(params, gradients, public[0].T, basis, partners.reshape(ROUNDS))

    w_spec = pl.BlockSpec((1, tile, columns), lambda i: (0, i, 0))
    weights, coefs, drift, norm = pl.pallas_call(
        blend,
        grid=(steps,),
        in_specs=[w_spec, pl.BlockSpec((tile, lanes), lambda i: (i, 0)),
                  pl.BlockSpec((rank, columns), lambda i: (0, 0)), VMEM],
        out_specs=[w_spec, pl.BlockSpec((rank, tile), lambda i: (0, i)), SMEM, SMEM],
        out_shape=[jax.ShapeDtypeStruct(params.shape, F32), jax.ShapeDtypeStruct((rank, height), F32),
                   jax.ShapeDtypeStruct((ROUNDS,), F32), jax.ShapeDtypeStruct((ROUNDS,), F32)],
        scratch_shapes=[pltpu.VMEM((3 * rank, columns), BF16)],
        compiler_params=pltpu.CompilerParams(dimension_semantics=("arbitrary",)),
        name="blend",
    )(half, final.reshape(height, lanes), basis, stats)
    return (weights, coefs.T[None], drift, norm)


def solution(mesh):
    return jax.shard_map(
        body,
        mesh=mesh,
        in_specs=(
            P("gossip", None, "mp"),
            P("gossip", None, None),
            P(None, "gossip", None, "mp"),
            P("mp", None),
            P(None, "gossip"),
        ),
        out_specs=(P("gossip", None, "mp"), P("gossip", None, None), P(), P()),
        check_vma=False,
    )
```
